64 devices in a mesh: dp: 4 (over x, y), dcp: 16 (over z, core).
Axes of the slice: x: 2, y: 2, z: 8, core: 2. Of those that a mesh axis runs over, the one named last changes fastest.
The devices are a block of a 4x4x8 slice.
Arguments:
- q_abs: bfloat16 [256, 64, 576], P('dp', 'dcp'), parts along dimension 0
- kv_cache: bfloat16 [256, 4, 16, 64, 576], P('dp', None, 'dcp'), parts along dimension 0
- lengths: int32 [256], P('dp'), parts along dimension 0
- w_uv: bfloat16 [64, 512, 128], replicated
Outputs:
- output: bfloat16 [256, 64, 128], P('dp', 'dcp'), parts along dimension 0
There are 4 independent parts. The reference program is written for one: setup_inputs(seed, part) draws one part's arguments, and reference() takes and returns one part's arrays. A program takes and returns all parts, laid end to end along the dimension named above; an argument that names none is the same for every part.
All inputs are finite; a program needn't handle non-finite values.
Results may differ from the reference program's by a relative error of at most 0.00935943.
Values are sent between devices in bfloat16 or wider.
A program may use at most 768 MiB of HBM per device.

```python
import jax
import jax.numpy as jnp
from jax import lax

BATCH = 64
HEADS = 64
LATENT = 512
ROPE = 64
VDIM = 128
PAGE = 64
PAGES_DEV = 4
GROUP = 16

KV_DIM = LATENT + ROPE
CTX = PAGES_DEV * GROUP * PAGE
QK_SCALE = (VDIM + ROPE) ** -0.5


def draw_lengths(key):
    key_short, key_full = jax.random.split(key)
    short_by = jax.random.randint(key_short, (BATCH,), 0, CTX // 2)
    full_row = jax.random.randint(key_full, (), 0, BATCH)
    lengths = jnp.where(jnp.arange(BATCH) == full_row, CTX, CTX - short_by)
    return lengths.astype(jnp.int32)


def setup_inputs(seed: int = 0, part: int = 0) -> dict:
    root_key = jax.random.key(seed)
    shared_key, part_root = jax.random.split(root_key)
    part_key = jax.random.fold_in(part_root, part)
    key_list = jax.random.split(part_key, 5)
    q_lat = jax.random.normal(key_list[0], (BATCH, HEADS, LATENT), jnp.float32)
    q_rot = 1.85 * jax.random.normal(key_list[1], (BATCH, HEADS, ROPE), jnp.float32)
    c_lat = jax.random.normal(key_list[2], (BATCH, PAGES_DEV, GROUP, PAGE, LATENT), jnp.float32)
    c_rot = 1.85 * jax.random.normal(key_list[3], (BATCH, PAGES_DEV, GROUP, PAGE, ROPE), jnp.float32)
    w_uv = jax.random.normal(shared_key, (HEADS, LATENT, VDIM), jnp.float32) * LATENT ** -0.5
    return {
        "q_abs": jnp.concatenate([q_lat, q_rot], axis=-1).astype(jnp.bfloat16),
        "kv_cache": jnp.concatenate([c_lat, c_rot], axis=-1).astype(jnp.bfloat16),
        "lengths": draw_lengths(key_list[4]),
        "w_uv": w_uv.astype(jnp.bfloat16),
    }


def reference(q_abs, kv_cache, lengths, w_uv):
    page_pos = (jnp.arange(PAGES_DEV)[:, None] * GROUP * PAGE + jnp.arange(PAGE)[None, :]).reshape(-1)

    def attend_seq(seq_args):
        q_row, c_row, length = seq_args

        def attend_dev(dev_idx):
            c_dev = lax.dynamic_index_in_dim(c_row, dev_idx, axis=1, keepdims=False)
            c_flat = c_dev.reshape(PAGES_DEV * PAGE, KV_DIM)
            valid_mask = page_pos + dev_idx * PAGE < length
            scores = jnp.dot(q_row, c_flat.T, preferred_element_type=jnp.float32) * QK_SCALE
            scores = jnp.where(valid_mask[None, :], scores, -jnp.inf)
            row_max = jnp.max(scores, axis=-1)
            exp_scores = jnp.exp(scores - row_max[:, None])
            row_sum = jnp.sum(exp_scores, axis=-1)
            o_part = jnp.dot(exp_scores.astype(jnp.bfloat16), c_flat[:, :LATENT], preferred_element_type=jnp.float32)
            o_part = (o_part / row_sum[:, None]).astype(jnp.bfloat16)
            return o_part, row_max + jnp.log(row_sum)

        o_parts, lse_parts = lax.map(attend_dev, jnp.arange(GROUP))
        lse_tot = jax.nn.logsumexp(lse_parts, axis=0)
        weight = jnp.exp(lse_parts - lse_tot[None, :])
        return jnp.sum(weight[:, :, None] * o_parts.astype(jnp.float32), axis=0)

    merged = lax.map(attend_seq, (q_abs, kv_cache, lengths))
    out_v = jnp.einsum("bhl,hlv->bhv", merged, w_uv.astype(jnp.float32))
    return out_v.astype(jnp.bfloat16)
```

```python
import functools

import jax
import jax.numpy as jnp
from jax import lax
from jax.experimental import pallas as pl
from jax.experimental.pallas import tpu as pltpu
from jax.sharding import PartitionSpec as P

MESH = pl.DeviceIdType.MESH
CHUNK_B = 8
GROUP_B = 4
UNIT_CH = 2
AHEAD = 3
LANES = 128


def kernel(dims, len_ref, q_hbm, kv_hbm, w_hbm, out_ref,
           qbuf, kvbuf, wbuf, obuf, lsebuf, vown, lown, vtw, ltw, vtr, ltr,
           va_in, la_in, vb_in, lb_in, va_out, la_out, vb_out, lb_out,
           q_sem, kv_sem, w_sem, a_send, b_send, t_send, a_recv, b_recv, t_recv,
           rt_send, rt_recv, ra_send, rb_send, ra_recv, rb_recv):
    (n_dev, head_loc, latent, rope, v_dim, pages_dev, page_len, n_batch, scale) = dims
    nz = n_dev // 2
    n_a, n_b = nz // 2, nz - 1 - nz // 2
    n_ch = n_batch // CHUNK_B
    n_unit = n_ch // UNIT_CH
    n_t = pages_dev * page_len
    n_lt = latent // LANES
    rows_ch = CHUNK_B * head_loc
    rows_g = GROUP_B * head_loc
    rows_u = rows_ch * UNIT_CH
    n_grp = CHUNK_B // GROUP_B

    me = lax.axis_index("dcp")
    z = me // 2
    c = me % 2
    sgn = 1 - 2 * c
    z_a = (z + sgn + nz) % nz
    z_b = (z - sgn + nz) % nz
    dev_a = {"dcp": z_a * 2 + c}
    dev_b = {"dcp": z_b * 2 + c}
    twin = {"dcp": z * 2 + 1 - c}

    def q_load(k):
        return pltpu.make_async_copy(q_hbm.at[k], qbuf.at[k, c, z], q_sem.at[k])

    def kv_load(k):
        part = pl.ds(k * CHUNK_B, CHUNK_B)
        return pltpu.make_async_copy(kv_hbm.at[part], kvbuf.at[part], kv_sem.at[k])

    w_load = pltpu.make_async_copy(w_hbm, wbuf, w_sem)

    for k in range(n_ch):
        q_load(k).start()

    barrier = pltpu.get_barrier_semaphore()
    for dev in (dev_a, dev_b, twin):
        pl.semaphore_signal(barrier, inc=1, device_id=dev, device_id_type=MESH)

    def remote(src, dst, send, recv, dev):
        return pltpu.make_async_remote_copy(
            src_ref=src, dst_ref=dst, send_sem=send, recv_sem=recv, device_id=dev, device_id_type=MESH)

    def q_send_a(k, slot, hop):
        ref = qbuf.at[k, c, slot]
        return remote(ref, ref, a_send, a_recv.at[k, hop], dev_a)

    def q_send_b(k, slot, hop):
        ref = qbuf.at[k, c, slot]
        return remote(ref, ref, b_send, b_recv.at[k, hop], dev_b)

    def q_send_t(k, slot):
        ref = qbuf.at[k, c, slot]
        return remote(ref, ref, t_send, t_recv.at[k], twin)

    def own_send(k):
        q_load(k).wait()
        q_send_a(k, z, 0).start()
        q_send_b(k, z, 0).start()
        q_send_t(k, z).start()

    def hop_a(k, hop):
        slot = (z - sgn * hop + nz) % nz
        q_send_a(k, slot, hop - 1).wait_recv()
        if hop < n_a:
            q_send_a(k, slot, hop).start()
        q_send_t(k, slot).start()

    def hop_b(k, hop):
        slot = (z + sgn * hop + nz) % nz
        q_send_b(k, slot, hop - 1).wait_recv()
        if hop < n_b:
            q_send_b(k, slot, hop).start()
        q_send_t(k, slot).start()

    def twin_wait(k):
        ref = qbuf.at[k, 1 - c]
        remote(ref, ref, t_send, t_recv.at[k], twin).wait_recv()

    sub8 = lax.broadcasted_iota(jnp.int32, (1, 8, 1), 1)
    first4 = sub8 < head_loc
    t_idx = lax.broadcasted_iota(jnp.int32, (1, 1, n_t), 2)
    pos = (t_idx // page_len * n_dev + me) * page_len + t_idx % page_len

    def attend(k, g):
        base = k * CHUNK_B + g * GROUP_B
        row0 = g * rows_g
        parts = []
        for j in range(n_lt):
            blk = qbuf[k, :, :, pl.ds(j * rows_ch + row0, rows_g), :]
            parts.append(blk.reshape(n_dev * rows_g, LANES))
        blk = qbuf[k, :, :, pl.ds(n_lt * rows_ch, rows_g), :]
        blk = blk.reshape(n_dev * rows_g, LANES)
        parts.append(blk[:, g * rope:(g + 1) * rope])
        lhs = jnp.concatenate(parts, axis=1)
        halves = []
        for b in range(GROUP_B):
            s = lax.dot_general(lhs, kvbuf[base + b], (((1,), (1,)), ((), ())),
                                preferred_element_type=jnp.float32)
            halves.append(s.reshape(n_dev, rows_g // 8, 8, n_t)[:, b // 2])
        outs, lses = [], []
        for p in range(GROUP_B // 2):
            b0 = base + 2 * p
            s = jnp.where(first4, halves[2 * p], halves[2 * p + 1]) * scale
            lim = jnp.where(first4, len_ref[b0], len_ref[b0 + 1])
            s = jnp.where(pos < lim, s, -jnp.inf)
            m = jnp.max(s, axis=-1, keepdims=True)
            e = jnp.exp(s - m)
            l = jnp.sum(e, axis=-1, keepdims=True)
            e0 = jnp.where(first4, e, 0.0).reshape(n_dev * 8, n_t)
            e1 = jnp.where(first4, 0.0, e).reshape(n_dev * 8, n_t)
            prob = jnp.concatenate([e0, e1], axis=1).astype(jnp.bfloat16)
            val = kvbuf[pl.ds(b0, 2), :, :latent].reshape(2 * n_t, latent)
            o = jnp.dot(prob, val, preferred_element_type=jnp.float32)
            outs.append(o.reshape(n_dev, 8, latent) / l)
            lses.append(jnp.broadcast_to(m + jnp.log(l), (n_dev, 8, LANES)))
        o = jnp.concatenate(outs, axis=1).astype(jnp.bfloat16)
        lse = jnp.concatenate(lses, axis=1)
        rows = pl.ds(pl.multiple_of((k % UNIT_CH) * rows_ch + row0, rows_g), rows_g)
        obuf[:, rows, :] = o
        lsebuf[:, rows, :] = lse

    eye = (lax.broadcasted_iota(jnp.int32, (rows_u, LANES), 0)
           == lax.broadcasted_iota(jnp.int32, (rows_u, LANES), 1))
    head_id = lax.broadcasted_iota(jnp.int32, (rows_u, 1), 0) % head_loc

    def expand(row):
        return jnp.sum(jnp.where(eye, row, 0.0), axis=1, keepdims=True)

    def project(slot, src_head):
        o = obuf[slot]
        w = jnp.concatenate([wbuf[src_head + h] for h in range(head_loc)], axis=1)
        full = jnp.dot(o, w, preferred_element_type=jnp.float32)
        v = full[:, :v_dim]
        for h in range(1, head_loc):
            v = jnp.where(head_id == h, full[:, h * v_dim:(h + 1) * v_dim], v)
        lse = jnp.sum(jnp.where(eye, lsebuf[slot], 0.0), axis=0, keepdims=True)
        return v, lse

    def twin_res(u):
        return (remote(vtw.at[u], vtr.at[u], rt_send.at[u, 0], rt_recv.at[u, 0], twin),
                remote(ltw.at[u], ltr.at[u], rt_send.at[u, 1], rt_recv.at[u, 1], twin))

    def project_unit(u):
        def other(i, _):
            v, lse = project((1 - c) * nz + i, (2 * i + 1 - c) * head_loc)
            vtw[u, i] = v
            ltw[u, pl.ds(i, 1), :] = lse
            return 0

        def own(i, _):
            v, lse = project(c * nz + i, (2 * i + c) * head_loc)
            vown[u, i] = v
            lown[u, pl.ds(i, 1), :] = lse
            return 0

        lax.fori_loop(0, nz, other, 0)
        for cp in twin_res(u):
            cp.start()
        lax.fori_loop(0, nz, own, 0)

    def weights(la, lb):
        m = jnp.maximum(la, lb)
        ea, eb = jnp.exp(la - m), jnp.exp(lb - m)
        s = ea + eb
        return ea / s, eb / s, m + jnp.log(s)

    def merge_twin(u):
        for cp in twin_res(u):
            cp.wait_recv()
        wa, wb, lse = weights(lown[u], ltr[u])
        for i in range(nz):
            vown[u, i] = expand(wa[i:i + 1]) * vown[u, i] + expand(wb[i:i + 1]) * vtr[u, i]
        lown[u] = lse

    def lse_row(u, dest):
        return lown[u, pl.ds(dest, 1), :]

    def res_a(u, hop):
        return (remote(va_out.at[u, hop], va_in.at[u, hop], ra_send.at[0], ra_recv.at[u, hop, 0], dev_a),
                remote(la_out.at[u, hop], la_in.at[u, hop], ra_send.at[1], ra_recv.at[u, hop, 1], dev_a))

    def res_b(u, hop):
        return (remote(vb_out.at[u, hop], vb_in.at[u, hop], rb_send.at[0], rb_recv.at[u, hop, 0], dev_b),
                remote(lb_out.at[u, hop], lb_in.at[u, hop], rb_send.at[1], rb_recv.at[u, hop, 1], dev_b))

    def step_dir(u, hop, n_hop, sign, res, v_in, l_in, v_out, l_out):
        dest = (z + sign * (n_hop - hop) + nz) % nz
        if hop == 0:
            v_out[u, 0] = vown[u, dest]
            l_out[u, 0] = lse_row(u, dest)
        else:
            for cp in res(u, hop - 1):
                cp.wait_recv()
            wa, wb, lse = weights(l_in[u, hop - 1], lse_row(u, dest))
            v_out[u, hop] = expand(wa) * v_in[u, hop - 1] + expand(wb) * vown[u, dest]
            l_out[u, hop] = lse
        return res(u, hop)

    def res_step(u, hop):
        cps = step_dir(u, hop, n_a, sgn, res_a, va_in, la_in, va_out, la_out)
        if hop < n_b:
            cps = cps + step_dir(u, hop, n_b, -sgn, res_b, vb_in, lb_in, vb_out, lb_out)
        for cp in cps:
            cp.start()

    def finish(u):
        for cp in res_a(u, n_a - 1) + res_b(u, n_b - 1):
            cp.wait_recv()
        wa, wb, lse = weights(la_in[u, n_a - 1], lb_in[u, n_b - 1])
        wc, wd, _ = weights(lse, lse_row(u, z))
        out = (expand(wa * wc) * va_in[u, n_a - 1] + expand(wb * wc) * vb_in[u, n_b - 1]
               + expand(wd) * vown[u, z])
        out_ref[pl.ds(pl.multiple_of(u * rows_u, rows_u), rows_u), :] = out.astype(out_ref.dtype)

    pl.semaphore_wait(barrier, 3)
    for k in range(AHEAD):
        own_send(k)
    for k in range(n_ch):
        kv_load(k).start()
    w_load.start()

    lag = (1, 3, 4, 6)
    n_round = n_ch + lag[-1]

    def when(cond, fn, *args):
        pl.when(cond)(lambda: fn(*args))

    def both(k, hop):
        def run():
            hop_a(k, hop)
            if hop <= n_b:
                hop_b(k, hop)
        pl.when((k >= 0) & (k < n_ch))(run)

    def round_body(r, _):
        both(r - lag[3], 4)
        both(r - lag[1], 2)
        when((r >= 1) & (r - 1 + AHEAD < n_ch), own_send, r - 1 + AHEAD)
        k = r - lag[3]

        def first_part():
            kv_load(k).wait()
            twin_wait(k)
            attend(k, 0)

        pl.when(k >= 0)(first_part)
        both(r - lag[2], 3)
        both(r - lag[0], 1)

        def second_part():
            for g in range(1, n_grp):
                attend(k, g)

        pl.when(k >= 0)(second_part)

        def unit_part():
            when(k == UNIT_CH - 1, w_load.wait)
            project_unit(k // UNIT_CH)

        pl.when((k >= 0) & (k % UNIT_CH == UNIT_CH - 1))(unit_part)

        def unit_merge():
            u = k // UNIT_CH - 1
            merge_twin(u)
            res_step(u, 0)

        pl.when((k >= UNIT_CH) & (k % UNIT_CH == 0))(unit_merge)
        return 0

    lax.fori_loop(1, n_round, round_body, 0)

    merge_twin(n_unit - 1)
    res_step(n_unit - 1, 0)
    for hop in range(1, n_a):
        def stage(u, _, hop=hop):
            res_step(u, hop)
            return 0
        lax.fori_loop(0, n_unit, stage, 0)

    def last(u, _):
        finish(u)
        return 0

    lax.fori_loop(0, n_unit, last, 0)

    ref = qbuf.at[:, 0, pl.ds(0, n_a)]
    remote(ref, ref, a_send, a_recv.at[0, 0], dev_a).wait_send()
    ref = qbuf.at[:, 0, pl.ds(0, n_b)]
    remote(ref, ref, b_send, b_recv.at[0, 0], dev_b).wait_send()
    ref = qbuf.at[:, 0]
    remote(ref, ref, t_send, t_recv.at[0], twin).wait_send()
    for u in range(n_unit):
        for cp in twin_res(u):
            cp.wait_send()
    remote(va_out, va_in, ra_send.at[0], ra_recv.at[0, 0, 0], dev_a).wait_send()
    remote(la_out, la_in, ra_send.at[1], ra_recv.at[0, 0, 1], dev_a).wait_send()
    remote(vb_out, vb_in, rb_send.at[0], rb_recv.at[0, 0, 0], dev_b).wait_send()
    remote(lb_out, lb_in, rb_send.at[1], rb_recv.at[0, 0, 1], dev_b).wait_send()


def solution(mesh):
    n_dev = mesh.shape["dcp"]

    def local_attend(q_own, kv_cache, lengths, w_uv):
        n_batch, pages_dev, _, page_len, kv_dim = kv_cache.shape
        head_loc = q_own.shape[1]
        latent, v_dim = w_uv.shape[1], w_uv.shape[2]
        rope = kv_dim - latent
        scale = (v_dim + rope) ** -0.5
        n_ch = n_batch // CHUNK_B
        n_unit = n_ch // UNIT_CH
        rows_ch = CHUNK_B * head_loc
        rows_u = rows_ch * UNIT_CH
        n_lt = latent // LANES
        nz = n_dev // 2
        n_a, n_b = nz // 2, nz - 1 - nz // 2
        n_grp = CHUNK_B // GROUP_B

        q = q_own.reshape(n_ch, rows_ch, kv_dim)
        lat = q[..., :latent].reshape(n_ch, rows_ch, n_lt, LANES).transpose(0, 2, 1, 3)
        lat = lat.reshape(n_ch, n_lt * rows_ch, LANES)
        rot = q[..., latent:].reshape(n_ch, n_grp, rows_ch // n_grp, rope).transpose(0, 2, 1, 3)
        rot = rot.reshape(n_ch, rows_ch // n_grp, n_grp * rope)
        q_msg = jnp.concatenate([lat, rot], axis=1)
        msg_rows = q_msg.shape[1]
        kv = kv_cache.reshape(n_batch, pages_dev * page_len, kv_dim)

        dims = (n_dev, head_loc, latent, rope, v_dim, pages_dev, page_len, n_batch, scale)
        f32, bf16 = jnp.float32, jnp.bfloat16
        dma = pltpu.SemaphoreType.DMA
        out = pl.pallas_call(
            functools.partial(kernel, dims),
            out_shape=jax.ShapeDtypeStruct((n_batch * head_loc, v_dim), bf16),
            in_specs=[
                pl.BlockSpec(memory_space=pltpu.SMEM),
                pl.BlockSpec(memory_space=pl.ANY),
                pl.BlockSpec(memory_space=pl.ANY),
                pl.BlockSpec(memory_space=pl.ANY),
            ],
            out_specs=pl.BlockSpec(memory_space=pltpu.VMEM),
            scratch_shapes=[
                pltpu.VMEM((n_ch, 2, nz, msg_rows, LANES), bf16),
                pltpu.VMEM(kv.shape, bf16),
                pltpu.VMEM(w_uv.shape, bf16),
                pltpu.VMEM((n_dev, rows_u, latent), bf16),
                pltpu.VMEM((n_dev, rows_u, LANES), f32),
                pltpu.VMEM((n_unit, nz, rows_u, v_dim), f32),
                pltpu.VMEM((n_unit, nz, LANES), f32),
                pltpu.VMEM((n_unit, nz, rows_u, v_dim), f32),
                pltpu.VMEM((n_unit, nz, LANES), f32),
                pltpu.VMEM((n_unit, nz, rows_u, v_dim), f32),
                pltpu.VMEM((n_unit, nz, LANES), f32),
                pltpu.VMEM((n_unit, n_a, rows_u, v_dim), f32),
                pltpu.VMEM((n_unit, n_a, 1, LANES), f32),
                pltpu.VMEM((n_unit, n_b, rows_u, v_dim), f32),
                pltpu.VMEM((n_unit, n_b, 1, LANES), f32),
                pltpu.VMEM((n_unit, n_a, rows_u, v_dim), f32),
                pltpu.VMEM((n_unit, n_a, 1, LANES), f32),
                pltpu.VMEM((n_unit, n_b, rows_u, v_dim), f32),
                pltpu.VMEM((n_unit, n_b, 1, LANES), f32),
                dma((n_ch,)),
                dma((n_ch,)),
                dma,
                dma,
                dma,
                dma,
                dma((n_ch, n_a)),
                dma((n_ch, n_b)),
                dma((n_ch,)),
                dma((n_unit, 2)),
                dma((n_unit, 2)),
                dma((2,)),
                dma((2,)),
                dma((n_unit, n_a, 2)),
                dma((n_unit, n_b, 2)),
            ],
            compiler_params=pltpu.CompilerParams(
                collective_id=0, has_side_effects=True, vmem_limit_bytes=60 * 1024 * 1024),
            name="mla_group",
        )(lengths, q_msg, kv, w_uv)
        return out.reshape(n_batch, head_loc, v_dim)

    return jax.shard_map(
        local_attend,
        mesh=mesh,
        in_specs=(P("dp", "dcp", None), P("dp", None, "dcp", None, None), P("dp"), P(None, None, None)),
        out_specs=P("dp", "dcp", None),
        check_vma=False,
    )
```

```python
import functools

import jax
import jax.numpy as jnp
from jax import lax
from jax.experimental import pallas as pl
from jax.experimental.pallas import tpu as pltpu
from jax.sharding import PartitionSpec as P

MESH = pl.DeviceIdType.MESH
CHUNK_B = 8
GROUP_B = 4
UNIT_CH = 2
LANES = 128
UNROLL = 4
ORDER = (
    (
        ("own", 0), ("own", 1), ("own", 2), ("own", 3), ("own", 4), ("own", 5), ("hop", 0, 1), ("hop", 1, 1),
        ("hop", 2, 1), ("hop", 4, 1), ("hop", 3, 1), ("hop", 0, 2), ("own", 6), ("hop", 1, 2), ("own", 7),
        ("hop", 2, 2), ("hop", 0, 3), ("hop", 5, 1), ("hop", 1, 3), ("hop", 3, 2), ("hop", 4, 2), ("hop", 2, 3),
        ("hop", 0, 4), ("hop", 5, 2), ("hop", 7, 1), ("hop", 6, 1), ("hop", 1, 4),
    ),
    (
        ("hop", 3, 3), ("hop", 4, 3),
    ),
    (
        ("hop", 5, 3), ("hop", 2, 4), ("hop", 6, 2), ("hop", 7, 2), ("s1", 0), ("hop", 3, 4),
    ),
    (
        ("hop", 4, 4),
    ),
    (
        ("hop", 6, 3), ("hop", 7, 3), ("hop", 5, 4),
    ),
    (

    ),
    (
        ("hop", 6, 4), ("s1", 1), ("hop", 7, 4), ("s2", 0), ("s1", 2),
    ),
    (

    ),
    (
        ("s1", 3), ("s2", 1), ("s2", 2), ("s2", 3), ("fin", 0), ("fin", 2), ("fin", 1), ("fin", 3),
    ),
)


def kernel(dims, len_ref, q_hbm, kv_hbm, w_hbm, out_ref,
           qbuf, kvbuf, wbuf, obuf, lsebuf, vown, lown, lrow, wmix, vtw, ltw, vtr, ltr,
           va_in, la_in, vb_in, lb_in, va_out, la_out, vb_out, lb_out,
           q_sem, kv_sem, w_sem, a_send, b_send, t_send, a_recv, b_recv, t_recv,
           rt_send, rt_recv, ra_send, rb_send, ra_recv, rb_recv):
    (n_dev, head_loc, latent, rope, v_dim, pages_dev, page_len, n_batch, scale) = dims
    nz = n_dev // 2
    n_a, n_b = nz // 2, nz - 1 - nz // 2
    n_ch = n_batch // CHUNK_B
    n_unit = n_ch // UNIT_CH
    n_t = pages_dev * page_len
    n_lt = latent // LANES
    rows_ch = CHUNK_B * head_loc
    rows_g = GROUP_B * head_loc
    rows_u = rows_ch * UNIT_CH
    n_grp = CHUNK_B // GROUP_B

    me = lax.axis_index("dcp")
    z = me // 2
    c = me % 2
    sgn = 1 - 2 * c

    def chip(dist):
        return (z + sgn * dist + nz) % nz

    dev_a, dev_b, dev_aa, dev_bb = ({"dcp": chip(d) * 2 + c} for d in (1, -1, 2, -2))
    twin = {"dcp": z * 2 + 1 - c}

    def q_load(k):
        return pltpu.make_async_copy(q_hbm.at[k], qbuf.at[k, c, z], q_sem.at[k])

    def kv_load(k):
        part = pl.ds(k * CHUNK_B, CHUNK_B)
        return pltpu.make_async_copy(kv_hbm.at[part], kvbuf.at[part], kv_sem.at[k])

    w_load = pltpu.make_async_copy(w_hbm, wbuf, w_sem)

    for k in range(n_ch):
        q_load(k).start()

    barrier = pltpu.get_barrier_semaphore()
    for dev in (dev_a, dev_b, dev_aa, dev_bb, twin):
        pl.semaphore_signal(barrier, inc=1, device_id=dev, device_id_type=MESH)

    def remote(src, dst, send, recv, dev):
        return pltpu.make_async_remote_copy(
            src_ref=src, dst_ref=dst, send_sem=send, recv_sem=recv, device_id=dev, device_id_type=MESH)

    def q_send_a(k, slot, hop):
        ref = qbuf.at[k, c, slot]
        return remote(ref, ref, a_send, a_recv.at[k, hop], dev_a)

    def q_send_b(k, slot, hop):
        ref = qbuf.at[k, c, slot]
        return remote(ref, ref, b_send, b_recv.at[k, hop], dev_b)

    def q_send_t(k, slot):
        ref = qbuf.at[k, c, slot]
        return remote(ref, ref, t_send, t_recv.at[k], twin)

    def own_send(k):
        q_load(k).wait()
        q_send_a(k, z, 0).start()
        q_send_b(k, z, 0).start()
        q_send_t(k, z).start()

    def hop_a(k, hop):
        slot = chip(-hop)
        q_send_a(k, slot, hop - 1).wait_recv()
        if hop < n_a:
            q_send_a(k, slot, hop).start()
        q_send_t(k, slot).start()

    def hop_b(k, hop):
        slot = chip(hop)
        q_send_b(k, slot, hop - 1).wait_recv()
        if hop < n_b:
            q_send_b(k, slot, hop).start()
        q_send_t(k, slot).start()

    def twin_wait(k):
        ref = qbuf.at[k, 1 - c]
        remote(ref, ref, t_send, t_recv.at[k], twin).wait_recv()

    sub8 = lax.broadcasted_iota(jnp.int32, (1, 8, 1), 1)
    first4 = sub8 < head_loc
    t_idx = lax.broadcasted_iota(jnp.int32, (1, 1, n_t), 2)
    pos = (t_idx // page_len * n_dev + me) * page_len + t_idx % page_len

    def attend(k, g):
        base = k * CHUNK_B + g * GROUP_B
        row0 = g * rows_g
        parts = []
        for j in range(n_lt):
            blk = qbuf[k, :, :, pl.ds(j * rows_ch + row0, rows_g), :]
            parts.append(blk.reshape(n_dev * rows_g, LANES))
        blk = qbuf[k, :, :, pl.ds(n_lt * rows_ch, rows_g), :]
        blk = blk.reshape(n_dev * rows_g, LANES)
        parts.append(blk[:, g * rope:(g + 1) * rope])
        lhs = jnp.concatenate(parts, axis=1)
        halves = []
        for b in range(GROUP_B):
            s = lax.dot_general(lhs, kvbuf[base + b], (((1,), (1,)), ((), ())),
                                preferred_element_type=jnp.float32)
            halves.append(s.reshape(n_dev, rows_g // 8, 8, n_t)[:, b // 2])
        outs, lses = [], []
        for p in range(GROUP_B // 2):
            b0 = base + 2 * p
            s = jnp.where(first4, halves[2 * p], halves[2 * p + 1]) * scale
            lim = jnp.where(first4, len_ref[b0], len_ref[b0 + 1])
            s = jnp.where(pos < lim, s, -jnp.inf)
            m = jnp.max(s, axis=-1, keepdims=True)
            e = jnp.exp(s - m)
            l = jnp.sum(e, axis=-1, keepdims=True)
            e0 = jnp.where(first4, e, 0.0).reshape(n_dev * 8, n_t)
            e1 = jnp.where(first4, 0.0, e).reshape(n_dev * 8, n_t)
            prob = jnp.concatenate([e0, e1], axis=1).astype(jnp.bfloat16)
            val = kvbuf[pl.ds(b0, 2), :, :latent].reshape(2 * n_t, latent)
            o = jnp.dot(prob, val, preferred_element_type=jnp.float32)
            outs.append(o.reshape(n_dev, 8, latent) / l)
            lses.append(jnp.broadcast_to(m + jnp.log(l), (n_dev, 8, LANES)))
        o = jnp.concatenate(outs, axis=1).astype(jnp.bfloat16)
        lse = jnp.concatenate(lses, axis=1)
        rows = pl.ds(pl.multiple_of((k % UNIT_CH) * rows_ch + row0, rows_g), rows_g)
        obuf[:, rows, :] = o
        lsebuf[:, rows, :] = lse

    eye = (lax.broadcasted_iota(jnp.int32, (rows_u, LANES), 0)
           == lax.broadcasted_iota(jnp.int32, (rows_u, LANES), 1))
    head_id = lax.broadcasted_iota(jnp.int32, (rows_u, 1), 0) % head_loc

    def expand(row):
        return jnp.sum(jnp.where(eye, row, 0.0), axis=1, keepdims=True)

    def project(slot, src_head):
        o = obuf[slot]
        w = jnp.concatenate([wbuf[src_head + h] for h in range(head_loc)], axis=1)
        full = jnp.dot(o, w, preferred_element_type=jnp.float32)
        v = full[:, :v_dim]
        for h in range(1, head_loc):
            v = jnp.where(head_id == h, full[:, h * v_dim:(h + 1) * v_dim], v)
        lse = jnp.sum(jnp.where(eye, lsebuf[slot], 0.0), axis=0, keepdims=True)
        return v, lse

    def twin_res(u):
        return (remote(vtw.at[u], vtr.at[u], rt_send.at[u, 0], rt_recv.at[u, 0], twin),
                remote(ltw.at[u], ltr.at[u], rt_send.at[u, 1], rt_recv.at[u, 1], twin))

    def project_unit(u):
        def side(cls, v_dst, l_dst):
            def run(i, _):
                for j in range(UNROLL):
                    d = i * UNROLL + j
                    v, lse = project(cls * nz + d, (2 * d + cls) * head_loc)
                    v_dst[u, d] = v
                    l_dst[u, pl.ds(d, 1), :] = lse
                return 0

            lax.fori_loop(0, nz // UNROLL, run, 0)

        side(1 - c, vtw, ltw)
        for cp in twin_res(u):
            cp.start()
        side(c, vown, lown)

    def merge(terms):
        top = functools.reduce(jnp.maximum, [l for _, l in terms])
        es = [jnp.exp(l - top) for _, l in terms]
        tot = functools.reduce(jnp.add, es)
        acc = functools.reduce(jnp.add, [expand(e / tot) * v for e, (v, _) in zip(es, terms)])
        return acc, top + jnp.log(tot)

    def copies(v_src, l_src, v_dst, l_dst, u, i, send, recv, dev):
        return (remote(v_src, v_dst.at[u, i], send.at[0], recv.at[u, i, 0], dev),
                remote(l_src, l_dst.at[u, i], send.at[1], recv.at[u, i, 1], dev))

    def send_a(u, i, v_src, l_src, dev):
        return copies(v_src, l_src, va_in, la_in, u, i, ra_send, ra_recv, dev)

    def send_b(u, i, v_src, l_src, dev):
        return copies(v_src, l_src, vb_in, lb_in, u, i, rb_send, rb_recv, dev)

    def wait_a(u, i):
        for cp in send_a(u, i, va_out.at[u], la_out.at[u], dev_a):
            cp.wait_recv()
        return va_in[u, i], la_in[u, i]

    def wait_b(u, i):
        for cp in send_b(u, i, vb_out.at[u], lb_out.at[u], dev_b):
            cp.wait_recv()
        return vb_in[u, i], lb_in[u, i]

    def stage_1(u):
        for cp in twin_res(u):
            cp.wait_recv()
        la, lb = lown[u], ltr[u]
        top = jnp.maximum(la, lb)
        ea, eb = jnp.exp(la - top), jnp.exp(lb - top)
        tot = ea + eb
        wmix[0] = ea / tot
        wmix[1] = eb / tot
        lown[u] = top + jnp.log(tot)

        def mix(dist):
            d = chip(dist)
            row = pl.ds(d, 1)
            vown[u, d] = expand(wmix[0, row, :]) * vown[u, d] + expand(wmix[1, row, :]) * vtr[u, d]
            lrow[u, d] = lown[u, row, :]

        def start(send, i, dist, dev):
            d = chip(dist)
            for cp in send(u, i, vown.at[u, d], lrow.at[u, d], dev):
                cp.start()

        for dist in (4, 3, -3):
            mix(dist)
        start(send_a, 0, 4, dev_aa)
        start(send_a, 1, 3, dev_a)
        start(send_b, 0, -3, dev_b)
        for dist in (1, -1):
            mix(dist)
        start(send_a, 2, 1, dev_a)
        start(send_b, 1, -1, dev_b)
        for dist in (2, -2, 0):
            mix(dist)

    def own_term(u, dist):
        d = chip(dist)
        return vown[u, d], lrow[u, d]

    def stage_2(u):
        va_out[u], la_out[u] = merge([wait_a(u, 0), wait_a(u, 1), own_term(u, 2)])
        vb_out[u], lb_out[u] = merge([wait_b(u, 0), own_term(u, -2)])
        for cp in send_a(u, 3, va_out.at[u], la_out.at[u], dev_aa) + send_b(u, 2, vb_out.at[u], lb_out.at[u], dev_bb):
            cp.start()

    def finish(u):
        out, _ = merge([wait_a(u, 2), wait_b(u, 1), wait_a(u, 3), wait_b(u, 2), own_term(u, 0)])
        out_ref[pl.ds(pl.multiple_of(u * rows_u, rows_u), rows_u), :] = out.astype(out_ref.dtype)

    def hop(k, h):
        hop_a(k, h)
        if h <= n_b:
            hop_b(k, h)

    steps = {"own": own_send, "hop": hop, "s1": stage_1, "s2": stage_2, "fin": finish}

    def run_steps(r):
        for step in ORDER[r]:
            steps[step[0]](*step[1:])

    pl.semaphore_wait(barrier, 5)
    for k in range(n_ch):
        kv_load(k).start()
    w_load.start()

    run_steps(0)

    def round_body(k, _):
        for r in range(1, n_ch):
            pl.when(k == r)(functools.partial(run_steps, r))
        kv_load(k).wait()
        twin_wait(k)
        for g in range(n_grp):
            attend(k, g)
        pl.when(k == UNIT_CH - 1)(lambda: w_load.wait())
        pl.when(k % UNIT_CH == UNIT_CH - 1)(lambda: project_unit(k // UNIT_CH))
        return 0

    lax.fori_loop(0, n_ch, round_body, 0)
    run_steps(n_ch)

    ref = qbuf.at[:, 0, pl.ds(0, n_a)]
    remote(ref, ref, a_send, a_recv.at[0, 0], dev_a).wait_send()
    ref = qbuf.at[:, 0, pl.ds(0, n_b)]
    remote(ref, ref, b_send, b_recv.at[0, 0], dev_b).wait_send()
    ref = qbuf.at[:, 0]
    remote(ref, ref, t_send, t_recv.at[0], twin).wait_send()
    for u in range(n_unit):
        for cp in twin_res(u):
            cp.wait_send()
    remote(va_in, va_in, ra_send.at[0], ra_recv.at[0, 0, 0], dev_a).wait_send()
    remote(la_in, la_in, ra_send.at[1], ra_recv.at[0, 0, 1], dev_a).wait_send()
    remote(vb_in, vb_in, rb_send.at[0], rb_recv.at[0, 0, 0], dev_b).wait_send()
    remote(lb_in, lb_in, rb_send.at[1], rb_recv.at[0, 0, 1], dev_b).wait_send()


def solution(mesh):
    n_dev = mesh.shape["dcp"]

    def local_attend(q_own, kv_cache, lengths, w_uv):
        n_batch, pages_dev, _, page_len, kv_dim = kv_cache.shape
        head_loc = q_own.shape[1]
        latent, v_dim = w_uv.shape[1], w_uv.shape[2]
        rope = kv_dim - latent
        scale = (v_dim + rope) ** -0.5
        n_ch = n_batch // CHUNK_B
        n_unit = n_ch // UNIT_CH
        rows_ch = CHUNK_B * head_loc
        rows_u = rows_ch * UNIT_CH
        n_lt = latent // LANES
        nz = n_dev // 2
        n_a, n_b = nz // 2, nz - 1 - nz // 2
        n_grp = CHUNK_B // GROUP_B

        q = q_own.reshape(n_ch, rows_ch, kv_dim)
        lat = q[..., :latent].reshape(n_ch, rows_ch, n_lt, LANES).transpose(0, 2, 1, 3)
        lat = lat.reshape(n_ch, n_lt * rows_ch, LANES)
        rot = q[..., latent:].reshape(n_ch, n_grp, rows_ch // n_grp, rope).transpose(0, 2, 1, 3)
        rot = rot.reshape(n_ch, rows_ch // n_grp, n_grp * rope)
        q_msg = jnp.concatenate([lat, rot], axis=1)
        msg_rows = q_msg.shape[1]
        kv = kv_cache.reshape(n_batch, pages_dev * page_len, kv_dim)

        dims = (n_dev, head_loc, latent, rope, v_dim, pages_dev, page_len, n_batch, scale)
        f32, bf16 = jnp.float32, jnp.bfloat16
        dma = pltpu.SemaphoreType.DMA
        out = pl.pallas_call(
            functools.partial(kernel, dims),
            out_shape=jax.ShapeDtypeStruct((n_batch * head_loc, v_dim), bf16),
            in_specs=[
                pl.BlockSpec(memory_space=pltpu.SMEM),
                pl.BlockSpec(memory_space=pl.ANY),
                pl.BlockSpec(memory_space=pl.ANY),
                pl.BlockSpec(memory_space=pl.ANY),
            ],
            out_specs=pl.BlockSpec(memory_space=pltpu.VMEM),
            scratch_shapes=[
                pltpu.VMEM((n_ch, 2, nz, msg_rows, LANES), bf16),
                pltpu.VMEM(kv.shape, bf16),
                pltpu.VMEM(w_uv.shape, bf16),
                pltpu.VMEM((n_dev, rows_u, latent), bf16),
                pltpu.VMEM((n_dev, rows_u, LANES), f32),
                pltpu.VMEM((n_unit, nz, rows_u, v_dim), f32),
                pltpu.VMEM((n_unit, nz, LANES), f32),
                pltpu.VMEM((n_unit, nz, 1, LANES), f32),
                pltpu.VMEM((2, nz, LANES), f32),
                pltpu.VMEM((n_unit, nz, rows_u, v_dim), f32),
                pltpu.VMEM((n_unit, nz, LANES), f32),
                pltpu.VMEM((n_unit, nz, rows_u, v_dim), f32),
                pltpu.VMEM((n_unit, nz, LANES), f32),
                pltpu.VMEM((n_unit, n_a, rows_u, v_dim), f32),
                pltpu.VMEM((n_unit, n_a, 1, LANES), f32),
                pltpu.VMEM((n_unit, n_b, rows_u, v_dim), f32),
                pltpu.VMEM((n_unit, n_b, 1, LANES), f32),
                pltpu.VMEM((n_unit, rows_u, v_dim), f32),
                pltpu.VMEM((n_unit, 1, LANES), f32),
                pltpu.VMEM((n_unit, rows_u, v_dim), f32),
                pltpu.VMEM((n_unit, 1, LANES), f32),
                dma((n_ch,)),
                dma((n_ch,)),
                dma,
                dma,
                dma,
                dma,
                dma((n_ch, n_a)),
                dma((n_ch, n_b)),
                dma((n_ch,)),
                dma((n_unit, 2)),
                dma((n_unit, 2)),
                dma((2,)),
                dma((2,)),
                dma((n_unit, n_a, 2)),
                dma((n_unit, n_b, 2)),
            ],
            compiler_params=pltpu.CompilerParams(
                collective_id=0, has_side_effects=True, vmem_limit_bytes=60 * 1024 * 1024),
            name="mla_group",
        )(lengths, q_msg, kv, w_uv)
        return out.reshape(n_batch, head_loc, v_dim)

    return jax.shard_map(
        local_attend,
        mesh=mesh,
        in_specs=(P("dp", "dcp", None), P("dp", None, "dcp", None, None), P("dp"), P(None, None, None)),
        out_specs=P("dp", "dcp", None),
        check_vma=False,
    )
```
